32 devices in a mesh: band: 16 (over z, x, core), lev: 2 (over y).
Axes of the slice: x: 2, y: 2, z: 4, core: 2. Of those that a mesh axis runs over, the one named last changes fastest.
Arguments:
- field_grid: float32 [3, 8, 384, 2, 1536], P(None, 'lev', 'band'), may hold values from -6 to 6
- increment: float32 [3, 8, 384, 2, 1536], P(None, 'lev', 'band'), may hold values from -6 to 6
- points: int32 [384], P('band'), may hold values from 16 to 1536, as said below
- weights: float32 [384], replicated, may hold values from 0.0013020834 to 0.0052083335
- pair_slot: int32 [384], replicated, may hold values from 0 to 383, each once
- legendre: float32 [384, 384, 769], P(('band', 'lev')), may hold values from -6 to 6
- strength: float32 [3, 8], replicated, may hold values from 1 to 16
Outputs:
- stepped: float32 [3, 8, 384, 2, 1536], P(None, 'lev', 'band')
The draws below stay inside these ranges and needn't reach their ends.
Inputs may be any that keep to these rules, and one draw needn't show every extreme that they name: points[j] lies within 32 of 16 + 1520 * j // 383, kept within 16 to 1536; the last latitude pair has 1536 cells. `pair_slot`: A permutation of 0 to 383; slot s is held by the device of joint band+lev index s // 12, at place s % 12, which holds legendre[s].
All inputs are finite; a program needn't handle non-finite values.
Results may differ from the reference program's by a relative error of at most 0.0003.
Values sent between devices are 32-bit elements; how exact they have to be, the bound alone decides.
A program may use at most 320 MiB of HBM per device.

```python
import math
import jax
import jax.numpy as jnp
from jax import lax

WAVES = 768
FIELDS = 3
HALF = 384
NLON = 1536
LEVELS = 8


def draw_points(key, part):
    pair_index = lax.iota(jnp.int32, HALF)
    smooth_count = 16 + (2 * WAVES - 16) * pair_index // (HALF - 1)
    jitter = jax.random.randint(key, (HALF,), -32, 33)
    counts = jnp.clip(smooth_count + jitter, 16, 2 * WAVES)
    return jnp.where(pair_index == HALF - 1, 2 * WAVES, counts).astype(jnp.int32)


def levels(own_key, dims, cuts, least, high):
    level, own = 1.0, jax.random.fold_in(own_key, 6)
    for position, shards_of in cuts:
        draws = jnp.exp(jax.random.uniform(jax.random.fold_in(own, position), (shards_of,), jnp.float32, least / len(cuts), high / len(cuts)))
        level = level * jnp.repeat(draws, dims[position] // shards_of).reshape([-1 if axis == position else 1 for axis in range(len(dims))])
    return level


def normal_values(rng, shape, spread, bound, cuts=(), kind=jnp.bfloat16):
    entries = jax.random.normal(rng, shape, jnp.float32) * spread
    if len(cuts) > 0:
        entries = levels(rng, shape, cuts, -0.22, 0.18) * entries
    return jnp.clip(entries, min=-bound, max=bound).astype(kind)


def setup_inputs(seed: int = 0) -> dict:
    arg_keys = jax.random.split(jax.random.key(seed), 8)
    return {
        "field_grid": normal_values(arg_keys[0], (FIELDS, LEVELS, HALF, 2, NLON), 1.0, 6.0, ((1, 2), (2, 16)), jnp.float32),
        "increment": normal_values(arg_keys[1], (FIELDS, LEVELS, HALF, 2, NLON), 1.0, 6.0, ((1, 2), (2, 16)), jnp.float32),
        "points": draw_points(jax.random.fold_in(arg_keys[7], 71), 0),
        "weights": jnp.clip(jnp.exp(jax.random.uniform(arg_keys[3], (HALF,), jnp.float32, math.log(0.0013020834), math.log(0.0052083335))), 0.0013020834, 0.0052083335),
        "pair_slot": jax.random.permutation(arg_keys[4], HALF).astype(jnp.int32),
        "legendre": normal_values(arg_keys[5], (HALF, HALF, WAVES + 1), 1.0, 6.0, ((0, 32),), jnp.float32),
        "strength": jnp.clip(jnp.exp(jax.random.uniform(arg_keys[6], (FIELDS, LEVELS), jnp.float32, math.log(1.0), math.log(16.0))), 1.0, 16.0),
    }


TWO_PI = 2.0 * math.pi


def dft_basis(count):
    places = lax.iota(jnp.int32, NLON)
    orders = lax.iota(jnp.int32, WAVES)
    turns = (places[:, None] * orders[None, :]) % count
    angle = turns.astype(jnp.float32) * (TWO_PI / count.astype(jnp.float32))
    live = (places[:, None] < count) & (orders[None, :] <= (count - 1) // 2)
    cosines = jnp.where(live, jnp.cos(angle), 0.0)
    sines = jnp.where(live, -jnp.sin(angle), 0.0)
    return jnp.concatenate([cosines, sines], axis=1)


def reference(field_grid, increment, points, weights, pair_slot, legendre, strength):
    summed = field_grid + increment
    row_count = FIELDS * LEVELS * 2
    by_pair = jnp.moveaxis(summed, 2, 0).reshape(HALF, row_count, NLON)

    def forward(item):
        block, count = item
        product = jnp.dot(block, dft_basis(count), precision=lax.Precision.HIGHEST)
        return product / count.astype(jnp.float32)

    spectra = lax.map(forward, (by_pair, points))
    spectra = spectra.reshape(HALF, FIELDS * LEVELS, 2, 2, WAVES)
    columns = lax.iota(jnp.int32, WAVES + 1)
    degree_top = float((WAVES - 1) * WAVES)
    damping_rate = strength.reshape(FIELDS * LEVELS)

    def per_pair(lower_wave):
        table = lax.dynamic_index_in_dim(legendre, pair_slot[lower_wave], 0, keepdims=False)
        higher_wave = WAVES - 1 - lower_wave
        first = lax.dynamic_index_in_dim(spectra, lower_wave, 4, keepdims=False)
        second = lax.dynamic_index_in_dim(spectra, higher_wave, 4, keepdims=False)
        second_member = columns >= WAVES - lower_wave
        degree = jnp.where(second_member, columns - 1, lower_wave + columns)
        wave_of_column = jnp.where(second_member, higher_wave, lower_wave)
        parity = jnp.where((degree - wave_of_column) % 2 == 0, 1.0, -1.0)
        first_weighted = (first * weights[:, None, None, None]).reshape(HALF, -1)
        second_weighted = (second * weights[:, None, None, None]).reshape(HALF, -1)
        part_first = jnp.dot(table.T, first_weighted, precision=lax.Precision.HIGHEST)
        part_second = jnp.dot(table.T, second_weighted, precision=lax.Precision.HIGHEST)
        part_first = part_first.reshape(WAVES + 1, FIELDS * LEVELS, 2, 2)
        part_second = part_second.reshape(WAVES + 1, FIELDS * LEVELS, 2, 2)
        chosen = jnp.where(second_member[:, None, None, None], part_second, part_first)
        coefficients = chosen[:, :, 0, :] + parity[:, None, None] * chosen[:, :, 1, :]
        degree_real = degree.astype(jnp.float32)
        degree_ratio = degree_real * (degree_real + 1.0) / degree_top
        damping = 1.0 / (1.0 + damping_rate[None, :] * (degree_ratio * degree_ratio)[:, None])
        damped = coefficients * damping[:, :, None]
        lower_part = jnp.where(second_member[:, None, None], 0.0, damped)
        upper_part = jnp.where(second_member[:, None, None], damped, 0.0)
        stacked = jnp.stack([lower_part, lower_part * parity[:, None, None],
                             upper_part, upper_part * parity[:, None, None]], axis=1)
        returned = jnp.dot(table, stacked.reshape(WAVES + 1, -1), precision=lax.Precision.HIGHEST)
        returned = returned.reshape(HALF, 2, 2, FIELDS * LEVELS, 2)
        return returned[:, 0], returned[:, 1]

    first_back, second_back = lax.map(per_pair, lax.iota(jnp.int32, HALF))
    by_wave = jnp.concatenate([first_back, second_back[::-1]], axis=0)
    spectral_rows = jnp.transpose(by_wave, (1, 3, 2, 4, 0)).reshape(HALF, row_count, 2 * WAVES)
    doubling = jnp.where(lax.iota(jnp.int32, 2 * WAVES) % WAVES == 0, 1.0, 2.0)

    def inverse(item):
        block, count = item
        return jnp.dot(block * doubling[None, :], dft_basis(count).T, precision=lax.Precision.HIGHEST)

    grid_rows = lax.map(inverse, (spectral_rows, points))
    grid_rows = grid_rows.reshape(HALF, FIELDS, LEVELS, 2, NLON)
    return jnp.moveaxis(grid_rows, 0, 2)
```

```python
import functools
import math

import jax
import jax.numpy as jnp
from jax import lax
from jax.experimental import pallas as pl
from jax.experimental.pallas import tpu as pltpu
from jax.sharding import PartitionSpec as P

LANES = 128
SPAN = 256
FINE = 16
MIB = 1024 * 1024
SINE = [(-1) ** k * math.pi ** (2 * k + 1) / math.factorial(2 * k + 1) for k in range(6)]
COSINE = [(-1) ** k * math.pi ** (2 * k) / math.factorial(2 * k) for k in range(7)]


def halves(values):
    high = values.astype(jnp.bfloat16)
    return high, (values - high.astype(jnp.float32)).astype(jnp.bfloat16)


def iota(shape, dim):
    return lax.broadcasted_iota(jnp.int32, shape, dim)


def turn(product, count, inverse):
    whole = jnp.floor(product * inverse + 0.5)
    part = (product - whole * count) * inverse
    square = part * part
    sine, cosine = SINE[-1], COSINE[-1]
    for term in SINE[-2::-1]:
        sine = sine * square + term
    for term in COSINE[-2::-1]:
        cosine = cosine * square + term
    sine = sine * part
    return 1.0 - 2.0 * sine * sine, 2.0 * sine * cosine


def dot(left, right):
    return lax.dot_general(
        left, right, (((1,), (0,)), ((), ())), preferred_element_type=jnp.float32
    )


def mirror(values):
    lane = iota(values.shape, 1)
    width = values.shape[1]
    return jnp.where(
        lane % 2 == 0,
        values + pltpu.roll(values, width - 1, 1),
        pltpu.roll(values, 1, 1) - values,
    )


def wave_at(pairs, place, waves):
    lower = pairs[place // 2]
    return jnp.where(place % 2 == 0, lower, waves - 1 - lower)


def forward_kernel(
    counts, pairs, field_ref, more_ref, out_ref, row_ref, high_ref, low_ref, wave_ref, *, stride
):
    fields, local, _, _, length = field_ref.shape
    devices, _, groups, lats, _ = out_ref.shape
    waves = length // 2
    rows = fields * local * 2
    each = 2 * local
    wide = 2 * each
    group = 2 * (waves // 2 // devices) // groups
    blocks = length // SPAN
    lat = pl.program_id(0)
    count = counts[lat]
    real = count.astype(jnp.float32)
    inverse = 1.0 / jnp.full((1, 1), real, jnp.float32)
    for f in range(fields):
        for l in range(local):
            row_ref[pl.ds((f * local + l) * 2, 2), :] = field_ref[f, l, 0] + more_ref[f, l, 0]
    pieces = []
    for b in range(blocks):
        piece = row_ref[:, b * SPAN : (b + 1) * SPAN]
        place = b * SPAN + iota(piece.shape, 1)
        pieces.append(jnp.where(place < count, piece, 0.0))
    high, low = halves(jnp.concatenate(pieces, axis=0))
    both = jnp.concatenate([high, low], axis=0)
    total = blocks * rows
    for q in range(waves // SPAN):
        order = q * SPAN + iota((1, SPAN), 1)
        order = order.astype(jnp.float32)
        steps = iota((FINE, SPAN), 0).astype(jnp.float32)
        fine_cos, fine_sin = turn(steps * order, real, inverse)
        coarse_cos, coarse_sin = turn(FINE * steps * order, real, inverse)
        block_cos, block_sin = turn(SPAN * steps[:8] * order, real, inverse)
        for i in range(SPAN // FINE):
            cosine, sine = coarse_cos[i : i + 1], coarse_sin[i : i + 1]
            place = pl.ds(i * FINE, FINE)
            top, rest = halves(cosine * fine_cos - sine * fine_sin)
            high_ref[q, place, :SPAN] = top
            low_ref[q, place, :SPAN] = rest
            top, rest = halves(sine * fine_cos + cosine * fine_sin)
            high_ref[q, place, SPAN:] = top
            low_ref[q, place, SPAN:] = rest
        first = dot(both, high_ref[q])
        product = first[:total] + (first[total:] + dot(high, low_ref[q]))
        real_part = jnp.zeros((rows, SPAN), jnp.float32)
        imaginary = jnp.zeros((rows, SPAN), jnp.float32)
        for b in range(blocks):
            in_cos = product[b * rows : (b + 1) * rows, :SPAN]
            in_sin = product[b * rows : (b + 1) * rows, SPAN:]
            cosine, sine = block_cos[b : b + 1], block_sin[b : b + 1]
            real_part += cosine * in_cos - sine * in_sin
            imaginary -= sine * in_cos + cosine * in_sin
        live = order.astype(jnp.int32) <= (count - 1) // 2
        scale = jnp.where(live, inverse, 0.0)
        real_part, imaginary = real_part * scale, imaginary * scale
        parts = []
        for f in range(fields):
            parts += [real_part[f * each : (f + 1) * each], imaginary[f * each : (f + 1) * each]]
        parts.append(jnp.zeros((LANES - fields * wide, SPAN), jnp.float32))
        turned = jnp.concatenate(parts, axis=0).T
        wave_ref[pl.ds(q * SPAN * stride + lat, SPAN, stride=stride), :] = turned

    @pl.when(lat == pl.num_programs(0) - 1)
    def _():
        lane = iota((lats, LANES), 1) // wide

        def assemble(index, carry):
            device, part = index // groups, index % groups
            outs = [jnp.zeros((lats, LANES), jnp.float32)] * fields
            for i in range(group):
                wave = wave_at(pairs, index * group + i, waves)
                value = wave_ref[pl.ds(pl.multiple_of(wave * stride, 8), lats), :]
                for f in range(fields):
                    moved = pltpu.roll(value, (i - f) * wide % LANES, 1)
                    outs[f] = jnp.where(lane == i, moved, outs[f])
            for f in range(fields):
                out_ref[device, f, part] = outs[f]
            return carry

        lax.fori_loop(0, devices * groups, assemble, 0)


def inverse_kernel(
    counts, pairs, come_ref, out_ref, high_ref, low_ref, wave_ref, *, stride
):
    fields, local, _, _, length = out_ref.shape
    devices, _, groups, lats, _ = come_ref.shape
    waves = length // 2
    rows = fields * local * 2
    each = 2 * local
    wide = 2 * each
    group = 2 * (waves // 2 // devices) // groups
    blocks = length // SPAN
    lat = pl.program_id(0)
    count = counts[lat]
    real = count.astype(jnp.float32)
    inverse = 1.0 / jnp.full((1, 1), real, jnp.float32)

    @pl.when(lat == 0)
    def _():
        lane = iota((lats, LANES), 1) // wide

        def spread(index, carry):
            device, part = index // groups, index % groups
            values = [come_ref[device, f, part] for f in range(fields)]
            for i in range(group):
                wave = wave_at(pairs, index * group + i, waves)
                out = jnp.zeros((lats, LANES), jnp.float32)
                for f in range(fields):
                    moved = pltpu.roll(values[f], (f - i) * wide % LANES, 1)
                    out = jnp.where(lane == f, moved, out)
                wave_ref[pl.ds(pl.multiple_of(wave * stride, 8), lats), :] = out
            return carry

        lax.fori_loop(0, devices * groups, spread, 0)

    total = blocks * rows
    result = jnp.zeros((total, SPAN), jnp.float32)
    place = iota((1, SPAN), 1).astype(jnp.float32)
    steps = iota((FINE, SPAN), 0).astype(jnp.float32)
    fine_cos, fine_sin = turn(steps * place, real, inverse)
    for q in range(waves // SPAN):
        start = float(q * SPAN)
        coarse_cos, coarse_sin = turn((start + FINE * steps) * place, real, inverse)
        order = start + place
        block_cos, block_sin = turn(SPAN * steps[:8] * order, real, inverse)
        for i in range(SPAN // FINE):
            cosine, sine = coarse_cos[i : i + 1], coarse_sin[i : i + 1]
            top, rest = halves(cosine * fine_cos - sine * fine_sin)
            high_ref[q, i * FINE : (i + 1) * FINE] = top
            low_ref[q, i * FINE : (i + 1) * FINE] = rest
            top, rest = halves(-(sine * fine_cos + cosine * fine_sin))
            high_ref[q, SPAN + i * FINE : SPAN + (i + 1) * FINE] = top
            low_ref[q, SPAN + i * FINE : SPAN + (i + 1) * FINE] = rest
        turned = wave_ref[pl.ds(q * SPAN * stride + lat, SPAN, stride=stride), :].T
        real_part = jnp.concatenate(
            [turned[f * wide : f * wide + each] for f in range(fields)], axis=0
        )
        imaginary = jnp.concatenate(
            [turned[f * wide + each : (f + 1) * wide] for f in range(fields)], axis=0
        )
        wave = order.astype(jnp.int32)
        double = jnp.where(wave == 0, 1.0, 2.0)
        double = jnp.where(wave <= (count - 1) // 2, double, 0.0)
        block_cos, block_sin = block_cos * double, block_sin * double
        shifted = []
        for b in range(blocks):
            cosine, sine = block_cos[b : b + 1], block_sin[b : b + 1]
            shifted.append(
                jnp.concatenate(
                    [real_part * cosine - imaginary * sine, real_part * sine + imaginary * cosine],
                    axis=1,
                )
            )
        high, low = halves(jnp.concatenate(shifted, axis=0))
        first = dot(jnp.concatenate([high, low], axis=0), high_ref[q])
        result += first[:total] + (first[total:] + dot(high, low_ref[q]))
    for b in range(blocks):
        live = b * SPAN + iota((rows, SPAN), 1) < count
        piece = jnp.where(live, result[b * rows : (b + 1) * rows], 0.0)
        for f in range(fields):
            for l in range(local):
                start = (f * local + l) * 2
                out_ref[f, l, 0, :, b * SPAN : (b + 1) * SPAN] = piece[start : start + 2]


def table_kernel(table_ref, weight_ref, high_ref, low_ref, high_t_ref, low_t_ref, pad_ref):
    columns = table_ref.shape[2]
    padded = pad_ref.shape[1]
    kept = high_t_ref.shape[1]
    pad_ref[:, padded - LANES :] = jnp.zeros((pad_ref.shape[0], LANES), jnp.float32)
    pad_ref[:, :columns] = table_ref[0]
    values = pad_ref[...]
    high_ref[0], low_ref[0] = halves(values)
    turned = values.T[:kept] * weight_ref[...]
    high_t_ref[0], low_t_ref[0] = halves(turned)


def legendre_kernel(
    lowers, come_ref, high_ref, low_ref, high_t_ref, low_t_ref, rate_ref, out_ref, data_ref, damp_ref,
    *, lev, waves, member
):
    slot = pl.program_id(0)
    devices, fields, _, lats, _ = come_ref.shape
    bands = devices // lev
    size = 2 * member
    per_tile = LANES // size
    pieces = lev * fields
    tiles = -(-pieces // per_tile)
    width = tiles * LANES
    lower = lowers[slot]
    spot = lowers[pl.num_programs(0) + slot]
    lane_piece = iota((lats, LANES), 1) // size
    for band in range(bands):
        for t in range(tiles):
            value = jnp.zeros((lats, LANES), jnp.float32)
            for k in range(t * per_tile, min((t + 1) * per_tile, pieces)):
                piece = come_ref[band * lev + k // fields, k % fields, 0]
                shift = lax.rem((k % per_tile) * size - spot * size + LANES, LANES)
                value = jnp.where(lane_piece == k % per_tile, pltpu.roll(piece, shift, 1), value)
            data_ref[pl.ds(band * lats, lats), t * LANES : (t + 1) * LANES] = value
    high, low = halves(mirror(data_ref[...]))
    kept = high_t_ref.shape[1]
    first = dot(high_t_ref[0], jnp.concatenate([high, low], axis=1))
    analysed = first[:, :width] + (first[:, width:] + dot(low_t_ref[0], high))
    column = iota((kept, 1), 0)
    second = column >= waves - lower
    degree = jnp.where(second, column - 1, lower + column)
    order = jnp.where(second, waves - 1 - lower, lower)
    odd = (degree - order) & 1
    code = jnp.where(column <= waves, 2 * second.astype(jnp.int32) + odd, -1)
    degree = degree.astype(jnp.float32)
    ratio = degree * (degree + 1.0) * (1.0 / float((waves - 1) * waves))
    square = ratio * ratio
    lane = iota((1, width), 1)
    mine = (lane // member % 2) * 2 + lane % 2
    damped = jnp.where(code == mine, analysed / (1.0 + rate_ref[...] * square), 0.0)
    damp_ref[:kept] = damped
    damp_ref[kept:] = jnp.zeros((damp_ref.shape[0] - kept, width), jnp.float32)
    high, low = halves(damp_ref[...])
    first = dot(high_ref[0], jnp.concatenate([high, low], axis=1))
    back = first[:, :width] + (first[:, width:] + dot(low_ref[0], high))
    data_ref[...] = mirror(back)

    @pl.when(spot == 0)
    def _():
        out_ref[...] = jnp.zeros_like(out_ref)

    for band in range(bands):
        for k in range(pieces):
            t = k // per_tile
            piece = data_ref[pl.ds(band * lats, lats), t * LANES : (t + 1) * LANES]
            shift = lax.rem(spot * size - (k % per_tile) * size + LANES, LANES)
            target = (band * lev + k // fields, k % fields, 0)
            out_ref[target] = jnp.where(lane_piece == spot, pltpu.roll(piece, shift, 1), out_ref[target])


def body(field_grid, increment, points, weights, pair_slot, legendre, strength):
    bands = lax.axis_size("band")
    lev = lax.axis_size("lev")
    devices = bands * lev
    fields, local, lats, _, length = field_grid.shape
    waves = length // 2
    slots, half, columns = legendre.shape
    member = 4 * local
    pair_count = waves // 2
    ranks = lax.iota(jnp.int32, pair_count)
    pairs = jnp.sum(jnp.where(pair_slot[None, :] == ranks[:, None], ranks[None, :], 0), axis=1)
    group = max(
        g for g in range(2, 2 * slots + 1, 2) if 2 * slots % g == 0 and g * member <= LANES
    )
    groups = 2 * slots // group
    stride = -(-lats // 8) * 8
    blocks = length // SPAN
    rows = fields * local * 2
    grid_block = pl.BlockSpec((fields, local, 1, 2, length), lambda j, *_: (0, 0, j, 0, 0))
    buffer = (devices, fields, groups, lats, LANES)
    whole_block = pl.BlockSpec(buffer, lambda j, *_: (0, 0, 0, 0, 0))
    waved = pltpu.VMEM((waves * stride, LANES), jnp.float32)
    flops = lats * 6 * blocks * rows * SPAN * length
    sent = pl.pallas_call(
        functools.partial(forward_kernel, stride=stride),
        out_shape=jax.ShapeDtypeStruct(buffer, jnp.float32),
        grid_spec=pltpu.PrefetchScalarGridSpec(
            num_scalar_prefetch=2,
            grid=(lats,),
            in_specs=[grid_block, grid_block],
            out_specs=whole_block,
            scratch_shapes=[
                pltpu.VMEM((rows, length), jnp.float32),
                pltpu.VMEM((waves // SPAN, SPAN, 2 * SPAN), jnp.bfloat16),
                pltpu.VMEM((waves // SPAN, SPAN, 2 * SPAN), jnp.bfloat16),
                waved,
            ],
        ),
        cost_estimate=pl.CostEstimate(flops=flops, bytes_accessed=0, transcendentals=0),
    )(points, pairs, field_grid, increment)
    arrived = lax.all_to_all(sent, ("band", "lev"), split_axis=0, concat_axis=0, tiled=True)

    padded = -(-columns // LANES) * LANES
    kept = -(-columns // 16) * 16
    plain = pl.BlockSpec((1, half, padded), lambda s, *_: (s, 0, 0))
    turned = pl.BlockSpec((1, kept, half), lambda s, *_: (s, 0, 0))
    tables = pl.pallas_call(
        table_kernel,
        out_shape=[jax.ShapeDtypeStruct((slots, half, padded), jnp.bfloat16)] * 2
        + [jax.ShapeDtypeStruct((slots, kept, half), jnp.bfloat16)] * 2,
        grid=(slots,),
        in_specs=[
            pl.BlockSpec((1, half, columns), lambda s: (s, 0, 0)),
            pl.BlockSpec((1, half), lambda s: (0, 0)),
        ],
        out_specs=[plain, plain, turned, turned],
        scratch_shapes=[pltpu.VMEM((half, padded), jnp.float32)],
        cost_estimate=pl.CostEstimate(
            flops=slots * 4 * half * padded * 256, bytes_accessed=0, transcendentals=0
        ),
    )(legendre, weights[None, :])

    size = 2 * member
    per_tile = LANES // size
    tiles = -(-lev * fields // per_tile)
    width = tiles * LANES
    rate = jnp.moveaxis(strength.reshape(fields, lev, local), 1, 0)
    rate = jnp.broadcast_to(rate[:, :, None, :, None], (lev, fields, 4, local, 2)).reshape(1, -1)
    rate = jnp.pad(rate, ((0, 0), (0, width - rate.shape[1])))
    own = lax.dynamic_slice_in_dim(pairs, lax.axis_index(("band", "lev")) * slots, slots)
    per_group = group // 2
    lowers = jnp.concatenate([own, lax.iota(jnp.int32, slots) % per_group])
    mail = pl.BlockSpec((devices, fields, 1, lats, LANES), lambda s, *_: (0, 0, s // per_group, 0, 0))
    returned = pl.pallas_call(
        functools.partial(legendre_kernel, lev=lev, waves=waves, member=member),
        out_shape=jax.ShapeDtypeStruct(buffer, jnp.float32),
        grid_spec=pltpu.PrefetchScalarGridSpec(
            num_scalar_prefetch=1,
            grid=(slots,),
            in_specs=[
                mail, plain, plain, turned, turned,
                pl.BlockSpec((1, width), lambda s, *_: (0, 0)),
            ],
            out_specs=mail,
            scratch_shapes=[
                pltpu.VMEM((half, width), jnp.float32),
                pltpu.VMEM((padded, width), jnp.float32),
            ],
        ),
        cost_estimate=pl.CostEstimate(
            flops=slots * 12 * half * padded * width, bytes_accessed=0, transcendentals=0
        ),
    )(lowers, arrived, *tables, rate)
    home = lax.all_to_all(returned, ("band", "lev"), split_axis=0, concat_axis=0, tiled=True)

    return pl.pallas_call(
        functools.partial(inverse_kernel, stride=stride),
        out_shape=jax.ShapeDtypeStruct(field_grid.shape, jnp.float32),
        grid_spec=pltpu.PrefetchScalarGridSpec(
            num_scalar_prefetch=2,
            grid=(lats,),
            in_specs=[whole_block],
            out_specs=grid_block,
            scratch_shapes=[
                pltpu.VMEM((waves // SPAN, 2 * SPAN, SPAN), jnp.bfloat16),
                pltpu.VMEM((waves // SPAN, 2 * SPAN, SPAN), jnp.bfloat16),
                waved,
            ],
        ),
        cost_estimate=pl.CostEstimate(flops=flops, bytes_accessed=0, transcendentals=0),
    )(points, pairs, home)


def solution(mesh):
    return jax.shard_map(
        body,
        mesh=mesh,
        in_specs=(
            P(None, "lev", "band", None, None),
            P(None, "lev", "band", None, None),
            P("band"),
            P(),
            P(),
            P(("band", "lev"), None, None),
            P(),
        ),
        out_specs=P(None, "lev", "band", None, None),
        check_vma=False,
    )
```

```python
import functools
import math

import jax
import jax.numpy as jnp
import numpy as np
from jax import lax
from jax.experimental import pallas as pl
from jax.experimental.pallas import tpu as pltpu
from jax.sharding import PartitionSpec as P

LANES = 128
SPAN = 256
FINE = 16
SEATS = 4
SINE = [(-1) ** k * math.pi ** (2 * k + 1) / math.factorial(2 * k + 1) for k in range(6)]
COSINE = [(-1) ** k * math.pi ** (2 * k) / math.factorial(2 * k) for k in range(7)]


def halves(values):
    high = values.astype(jnp.bfloat16)
    return high, (values - high.astype(jnp.float32)).astype(jnp.bfloat16)


def iota(shape, dim):
    return lax.broadcasted_iota(jnp.int32, shape, dim)


def turn(product, count, inverse):
    whole = jnp.floor(product * inverse + 0.5)
    part = (product - whole * count) * inverse
    square = part * part
    sine, cosine = SINE[-1], COSINE[-1]
    for term in SINE[-2::-1]:
        sine = sine * square + term
    for term in COSINE[-2::-1]:
        cosine = cosine * square + term
    sine = sine * part
    return 1.0 - 2.0 * sine * sine, 2.0 * sine * cosine


def dot(left, right):
    return lax.dot_general(
        left, right, (((1,), (0,)), ((), ())), preferred_element_type=jnp.float32
    )


def mirror(values):
    lane = iota(values.shape, 1)
    width = values.shape[1]
    return jnp.where(
        lane % 2 == 0,
        values + pltpu.roll(values, width - 1, 1),
        pltpu.roll(values, 1, 1) - values,
    )


def forward_kernel(
    counts, pairs, field_ref, more_ref, out_ref, row_ref, high_ref, low_ref, wave_ref, *, stride
):
    fields, local, _, _, length = field_ref.shape
    chunks, devices, tiles, lats, _ = out_ref.shape
    waves = length // 2
    rows = fields * local * 2
    each = 2 * local
    wide = 2 * each
    group = waves // 2 // devices // chunks
    blocks = length // SPAN
    lat = pl.program_id(0)
    count = counts[lat]
    real = count.astype(jnp.float32)
    inverse = 1.0 / jnp.full((1, 1), real, jnp.float32)
    for f in range(fields):
        for l in range(local):
            row_ref[pl.ds((f * local + l) * 2, 2), :] = field_ref[f, l, 0] + more_ref[f, l, 0]
    pieces = []
    for b in range(blocks):
        piece = row_ref[:, b * SPAN : (b + 1) * SPAN]
        place = b * SPAN + iota(piece.shape, 1)
        pieces.append(jnp.where(place < count, piece, 0.0))
    high, low = halves(jnp.concatenate(pieces, axis=0))
    both = jnp.concatenate([high, low], axis=0)
    total = blocks * rows
    for q in range(waves // SPAN):
        order = q * SPAN + iota((1, SPAN), 1)
        order = order.astype(jnp.float32)
        steps = iota((FINE, SPAN), 0).astype(jnp.float32)
        fine_cos, fine_sin = turn(steps * order, real, inverse)
        coarse_cos, coarse_sin = turn(FINE * steps * order, real, inverse)
        block_cos, block_sin = turn(SPAN * steps[:8] * order, real, inverse)
        for i in range(SPAN // FINE):
            cosine, sine = coarse_cos[i : i + 1], coarse_sin[i : i + 1]
            place = pl.ds(i * FINE, FINE)
            top, rest = halves(cosine * fine_cos - sine * fine_sin)
            high_ref[q, place, :SPAN] = top
            low_ref[q, place, :SPAN] = rest
            top, rest = halves(sine * fine_cos + cosine * fine_sin)
            high_ref[q, place, SPAN:] = top
            low_ref[q, place, SPAN:] = rest
        first = dot(both, high_ref[q])
        product = first[:total] + (first[total:] + dot(high, low_ref[q]))
        real_part = jnp.zeros((rows, SPAN), jnp.float32)
        imaginary = jnp.zeros((rows, SPAN), jnp.float32)
        for b in range(blocks):
            in_cos = product[b * rows : (b + 1) * rows, :SPAN]
            in_sin = product[b * rows : (b + 1) * rows, SPAN:]
            cosine, sine = block_cos[b : b + 1], block_sin[b : b + 1]
            real_part += cosine * in_cos - sine * in_sin
            imaginary -= sine * in_cos + cosine * in_sin
        live = order.astype(jnp.int32) <= (count - 1) // 2
        scale = jnp.where(live, inverse, 0.0)
        real_part, imaginary = real_part * scale, imaginary * scale
        parts = []
        for f in range(fields):
            parts += [real_part[f * each : (f + 1) * each], imaginary[f * each : (f + 1) * each]]
        parts.append(jnp.zeros((LANES - fields * wide, SPAN), jnp.float32))
        turned = jnp.concatenate(parts, axis=0).T
        wave_ref[pl.ds(q * SPAN * stride + lat, SPAN, stride=stride), :] = turned

    @pl.when(lat == pl.num_programs(0) - 1)
    def _():
        lane = iota((lats, LANES), 1) // wide

        def assemble(index, carry):
            chunk, device = index // devices, index % devices
            outs = [jnp.zeros((lats, LANES), jnp.float32)] * tiles
            for s in range(group):
                lower = pairs[device * chunks * group + chunk * group + s]
                for member in range(2):
                    wave = lower if member == 0 else waves - 1 - lower
                    value = wave_ref[pl.ds(pl.multiple_of(wave * stride, 8), lats), :]
                    for f in range(fields):
                        unit = member * fields + f
                        spot = unit % 2 * SEATS + s
                        moved = pltpu.roll(value, (spot - f) * wide % LANES, 1)
                        outs[unit // 2] = jnp.where(lane == spot, moved, outs[unit // 2])
            for t in range(tiles):
                out_ref[chunk, device, t] = outs[t]
            return carry

        lax.fori_loop(0, devices * chunks, assemble, 0)


def inverse_kernel(
    counts, pairs, come_ref, out_ref, high_ref, low_ref, wave_ref, *, stride, light, short
):
    fields, local, _, _, length = out_ref.shape
    chunks, devices, tiles, lats, _ = come_ref.shape
    waves = length // 2
    rows = fields * local * 2
    each = 2 * local
    wide = 2 * each
    group = waves // 2 // devices // chunks
    blocks = length // SPAN
    lat = pl.program_id(0)
    count = counts[lat]
    real = count.astype(jnp.float32)
    inverse = 1.0 / jnp.full((1, 1), real, jnp.float32)

    @pl.when(lat == 0)
    def _():
        lane = iota((lats, LANES), 1) // wide
        small = lax.axis_index("band") < light

        def spread(index, carry):
            chunk, device = index // devices, index % devices
            values = [come_ref[chunk, device, t] for t in range(tiles)]
            for t in range(short, tiles):
                values[t] = jnp.where(small, 0.0, values[t])
            for s in range(group):
                lower = pairs[device * chunks * group + chunk * group + s]
                for member in range(2):
                    wave = lower if member == 0 else waves - 1 - lower
                    out = jnp.zeros((lats, LANES), jnp.float32)
                    for f in range(fields):
                        unit = member * fields + f
                        spot = unit % 2 * SEATS + s
                        moved = pltpu.roll(values[unit // 2], (f - spot) * wide % LANES, 1)
                        out = jnp.where(lane == f, moved, out)
                    wave_ref[pl.ds(pl.multiple_of(wave * stride, 8), lats), :] = out
            return carry

        lax.fori_loop(0, devices * chunks, spread, 0)

    total = blocks * rows
    result = jnp.zeros((total, SPAN), jnp.float32)
    place = iota((1, SPAN), 1).astype(jnp.float32)
    steps = iota((FINE, SPAN), 0).astype(jnp.float32)
    fine_cos, fine_sin = turn(steps * place, real, inverse)
    for q in range(waves // SPAN):
        start = float(q * SPAN)
        coarse_cos, coarse_sin = turn((start + FINE * steps) * place, real, inverse)
        order = start + place
        block_cos, block_sin = turn(SPAN * steps[:8] * order, real, inverse)
        for i in range(SPAN // FINE):
            cosine, sine = coarse_cos[i : i + 1], coarse_sin[i : i + 1]
            top, rest = halves(cosine * fine_cos - sine * fine_sin)
            high_ref[q, i * FINE : (i + 1) * FINE] = top
            low_ref[q, i * FINE : (i + 1) * FINE] = rest
            top, rest = halves(-(sine * fine_cos + cosine * fine_sin))
            high_ref[q, SPAN + i * FINE : SPAN + (i + 1) * FINE] = top
            low_ref[q, SPAN + i * FINE : SPAN + (i + 1) * FINE] = rest
        turned = wave_ref[pl.ds(q * SPAN * stride + lat, SPAN, stride=stride), :].T
        real_part = jnp.concatenate(
            [turned[f * wide : f * wide + each] for f in range(fields)], axis=0
        )
        imaginary = jnp.concatenate(
            [turned[f * wide + each : (f + 1) * wide] for f in range(fields)], axis=0
        )
        wave = order.astype(jnp.int32)
        double = jnp.where(wave == 0, 1.0, 2.0)
        double = jnp.where(wave <= (count - 1) // 2, double, 0.0)
        block_cos, block_sin = block_cos * double, block_sin * double
        shifted = []
        for b in range(blocks):
            cosine, sine = block_cos[b : b + 1], block_sin[b : b + 1]
            shifted.append(
                jnp.concatenate(
                    [real_part * cosine - imaginary * sine, real_part * sine + imaginary * cosine],
                    axis=1,
                )
            )
        high, low = halves(jnp.concatenate(shifted, axis=0))
        first = dot(jnp.concatenate([high, low], axis=0), high_ref[q])
        result += first[:total] + (first[total:] + dot(high, low_ref[q]))
    for b in range(blocks):
        live = b * SPAN + iota((rows, SPAN), 1) < count
        piece = jnp.where(live, result[b * rows : (b + 1) * rows], 0.0)
        for f in range(fields):
            for l in range(local):
                start = (f * local + l) * 2
                out_ref[f, l, 0, :, b * SPAN : (b + 1) * SPAN] = piece[start : start + 2]


def exchange_kernel(
    lowers, sent_ref, table_ref, weight_ref, rate_ref, mine_ref, home_ref,
    come_ref, back_ref, pad_ref, data_ref, out_sem, in_sem, back_out_sem, back_in_sem, own_sem,
    *, lev, waves, light, short,
):
    slot = pl.program_id(0)
    chunks, devices, tiles, lats, _ = come_ref.shape
    bands = devices // lev
    slots = pl.num_programs(0)
    group = waves // 2 // devices // chunks
    chunk, spot = slot // group, slot % group
    band = lax.axis_index("band")
    me = band * lev + lax.axis_index("lev")

    def message(source, target, send_sem, recv_sem, g, there, where, device, small):
        part = pl.ds(0, short if small else tiles)
        return pltpu.make_async_remote_copy(
            src_ref=source.at[g, there, part],
            dst_ref=target.at[g, where, part],
            send_sem=send_sem.at[g, there],
            recv_sem=recv_sem.at[g, where],
            device_id=(device // lev, device % lev),
            device_id_type=pl.DeviceIdType.MESH,
        )

    def each_other(act, g, small_of):
        def one(step, carry):
            other = lax.rem(me + step, devices)
            small = small_of(other)

            @pl.when(small)
            def _():
                act(g, other, True)

            @pl.when(jnp.logical_not(small))
            def _():
                act(g, other, False)

            return carry

        lax.fori_loop(1, devices, one, 0)

    def mine_small(other):
        return band < light

    def their_small(other):
        return other // lev < light

    def go(g, other, small):
        message(sent_ref, come_ref, out_sem, in_sem, g, other, me, other, small).start()

    def gone(g, other, small):
        message(sent_ref, come_ref, out_sem, in_sem, g, other, me, other, small).wait_send()

    def come(g, other, small):
        message(sent_ref, come_ref, out_sem, in_sem, g, other, other, other, small).wait_recv()

    def back_go(g, other, small):
        message(back_ref, home_ref, back_out_sem, back_in_sem, g, other, me, other, small).start()

    def back_gone(g, other, small):
        message(back_ref, home_ref, back_out_sem, back_in_sem, g, other, me, other, small).wait_send()

    def back_come(g, other, small):
        message(
            back_ref, home_ref, back_out_sem, back_in_sem, g, other, other, other, small
        ).wait_recv()

    def own(g):
        return pltpu.make_async_copy(sent_ref.at[g, me], come_ref.at[g, me], own_sem.at[g])

    def own_back(g):
        return pltpu.make_async_copy(
            back_ref.at[g, me], home_ref.at[g, me], own_sem.at[chunks + g]
        )

    @pl.when(slot == 0)
    def _():
        def begin(g, carry):
            own(g).start()
            each_other(go, g, mine_small)
            return carry

        lax.fori_loop(0, chunks, begin, 0)
        pad_ref[...] = jnp.zeros_like(pad_ref)

    columns = table_ref.shape[1]
    pad_ref[:columns] = table_ref[0]
    table_high, table_low = halves(pad_ref[...])

    @pl.when(spot == 0)
    def _():
        own(chunk).wait()
        each_other(come, chunk, their_small)

    arrays = lev * tiles
    wides = -(-arrays // SEATS)
    width = wides * LANES
    member = LANES // (2 * SEATS)
    seat = iota((lats, LANES), 1) // member % SEATS
    for b in range(bands):
        for w in range(wides):
            value = jnp.zeros((lats, LANES), jnp.float32)
            for k in range(w * SEATS, min((w + 1) * SEATS, arrays)):
                if b < light and k % tiles >= short:
                    continue
                piece = come_ref[chunk, b * lev + k // tiles, k % tiles]
                shift = lax.rem((k % SEATS - spot) * member + LANES, LANES)
                value = jnp.where(seat == k % SEATS, pltpu.roll(piece, shift, 1), value)
            data_ref[pl.ds(b * lats, lats), w * LANES : (w + 1) * LANES] = value
    weight = jnp.concatenate([weight_ref[...]] * wides, axis=1)
    high, low = halves(mirror(data_ref[...]) * weight)
    first = dot(table_high, jnp.concatenate([high, low], axis=1))
    analysed = first[:, :width] + (first[:, width:] + dot(table_low, high))
    lower = lowers[slot]
    column = iota((pad_ref.shape[0], 1), 0)
    second = column >= waves - lower
    degree = jnp.where(second, column - 1, lower + column)
    order = jnp.where(second, waves - 1 - lower, lower)
    odd = (degree - order) & 1
    code = jnp.where(column <= waves, 2 * second.astype(jnp.int32) + odd, -1)
    degree = degree.astype(jnp.float32)
    ratio = degree * (degree + 1.0) * (1.0 / float((waves - 1) * waves))
    square = ratio * ratio
    damped = jnp.where(code == mine_ref[...], analysed / (1.0 + rate_ref[...] * square), 0.0)
    high, low = halves(damped)
    first = dot(table_high.T, jnp.concatenate([high, low], axis=1))
    back = first[:, :width] + (first[:, width:] + dot(table_low.T, high))
    data_ref[...] = mirror(back)

    @pl.when(spot == 0)
    def _():
        back_ref[chunk] = jnp.zeros(back_ref.shape[1:], jnp.float32)

    for b in range(bands):
        for k in range(arrays):
            if b < light and k % tiles >= short:
                continue
            w = k // SEATS
            piece = data_ref[pl.ds(b * lats, lats), w * LANES : (w + 1) * LANES]
            shift = lax.rem((spot - k % SEATS) * member + LANES, LANES)
            target = (chunk, b * lev + k // tiles, k % tiles)
            back_ref[target] = jnp.where(seat == spot, pltpu.roll(piece, shift, 1), back_ref[target])

    @pl.when(spot == group - 1)
    def _():
        own_back(chunk).start()
        each_other(back_go, chunk, their_small)

    @pl.when(slot == slots - 1)
    def _():
        def end(g, carry):
            own_back(g).wait()
            each_other(back_come, g, mine_small)
            each_other(gone, g, mine_small)
            each_other(back_gone, g, their_small)
            return carry

        lax.fori_loop(0, chunks, end, 0)


def body(field_grid, increment, points, weights, pair_slot, legendre, strength):
    bands = lax.axis_size("band")
    lev = lax.axis_size("lev")
    devices = bands * lev
    fields, local, lats, _, length = field_grid.shape
    waves = length // 2
    slots, half, columns = legendre.shape
    member = 4 * local
    assert member * 2 * SEATS == LANES
    pair_count = waves // 2
    ranks = lax.iota(jnp.int32, pair_count)
    pairs = jnp.sum(jnp.where(pair_slot[None, :] == ranks[:, None], ranks[None, :], 0), axis=1)
    group = max(g for g in range(1, SEATS + 1) if slots % g == 0)
    chunks = slots // group
    tiles = fields
    short = (fields + 1) // 2
    most = [
        min(length, 48 + (length - 16) * (lats * (b + 1) - 1) // (half - 1)) for b in range(bands)
    ]
    light = sum((cells - 1) // 2 < pair_count for cells in most)
    stride = -(-lats // 8) * 8
    blocks = length // SPAN
    rows = fields * local * 2
    grid_block = pl.BlockSpec((fields, local, 1, 2, length), lambda j, *_: (0, 0, j, 0, 0))
    buffer = (chunks, devices, tiles, lats, LANES)
    whole_block = pl.BlockSpec(buffer, lambda j, *_: (0, 0, 0, 0, 0))
    waved = pltpu.VMEM((waves * stride, LANES), jnp.float32)
    flops = lats * 6 * blocks * rows * SPAN * length
    sent = pl.pallas_call(
        functools.partial(forward_kernel, stride=stride),
        out_shape=jax.ShapeDtypeStruct(buffer, jnp.float32),
        grid_spec=pltpu.PrefetchScalarGridSpec(
            num_scalar_prefetch=2,
            grid=(lats,),
            in_specs=[grid_block, grid_block],
            out_specs=whole_block,
            scratch_shapes=[
                pltpu.VMEM((rows, length), jnp.float32),
                pltpu.VMEM((waves // SPAN, SPAN, 2 * SPAN), jnp.bfloat16),
                pltpu.VMEM((waves // SPAN, SPAN, 2 * SPAN), jnp.bfloat16),
                waved,
            ],
        ),
        cost_estimate=pl.CostEstimate(flops=flops, bytes_accessed=0, transcendentals=0),
    )(points, pairs, field_grid, increment)

    arrays = lev * tiles
    width = -(-arrays // SEATS) * LANES
    padded = -(-columns // LANES) * LANES
    lane = np.arange(width)
    seat = lane % LANES // member
    array = lane // LANES * SEATS + seat % SEATS
    unit = array % tiles * 2 + seat // SEATS
    real = array < arrays
    mine = np.where(real, unit // fields * 2 + lane % 2, -2)
    level = array // tiles * local + lane // 2 % local
    rank = np.where(real, unit % fields * lev * local + level, 0)
    choice = jnp.asarray(np.arange(fields * lev * local)[:, None] == rank[None, :], jnp.float32)
    rate = jnp.sum(choice * strength.reshape(-1, 1), axis=0, keepdims=True)
    own = lax.dynamic_slice_in_dim(pairs, lax.axis_index(("band", "lev")) * slots, slots)
    home = pl.pallas_call(
        functools.partial(exchange_kernel, lev=lev, waves=waves, light=light, short=short),
        out_shape=jax.ShapeDtypeStruct(buffer, jnp.float32),
        grid_spec=pltpu.PrefetchScalarGridSpec(
            num_scalar_prefetch=1,
            grid=(slots,),
            in_specs=[
                pl.BlockSpec(memory_space=pl.ANY),
                pl.BlockSpec((1, columns, half), lambda s, *_: (s, 0, 0)),
                pl.BlockSpec((half, LANES), lambda s, *_: (0, 0)),
                pl.BlockSpec((1, width), lambda s, *_: (0, 0)),
                pl.BlockSpec((1, width), lambda s, *_: (0, 0)),
            ],
            out_specs=pl.BlockSpec(memory_space=pl.ANY),
            scratch_shapes=[
                pltpu.VMEM(buffer, jnp.float32),
                pltpu.VMEM(buffer, jnp.float32),
                pltpu.VMEM((padded, half), jnp.float32),
                pltpu.VMEM((half, width), jnp.float32),
                pltpu.SemaphoreType.DMA((chunks, devices)),
                pltpu.SemaphoreType.DMA((chunks, devices)),
                pltpu.SemaphoreType.DMA((chunks, devices)),
                pltpu.SemaphoreType.DMA((chunks, devices)),
                pltpu.SemaphoreType.DMA((2 * chunks,)),
            ],
        ),
        compiler_params=pltpu.CompilerParams(has_side_effects=True),
        cost_estimate=pl.CostEstimate(
            flops=slots * 12 * half * padded * width, bytes_accessed=0, transcendentals=0
        ),
    )(
        own,
        sent,
        jnp.swapaxes(legendre, 1, 2),
        jnp.broadcast_to(weights[:, None], (half, LANES)),
        rate,
        jnp.asarray(mine[None, :], jnp.int32),
    )

    return pl.pallas_call(
        functools.partial(inverse_kernel, stride=stride, light=light, short=short),
        out_shape=jax.ShapeDtypeStruct(field_grid.shape, jnp.float32),
        grid_spec=pltpu.PrefetchScalarGridSpec(
            num_scalar_prefetch=2,
            grid=(lats,),
            in_specs=[whole_block],
            out_specs=grid_block,
            scratch_shapes=[
                pltpu.VMEM((waves // SPAN, 2 * SPAN, SPAN), jnp.bfloat16),
                pltpu.VMEM((waves // SPAN, 2 * SPAN, SPAN), jnp.bfloat16),
                waved,
            ],
        ),
        cost_estimate=pl.CostEstimate(flops=flops, bytes_accessed=0, transcendentals=0),
    )(points, pairs, home)


def solution(mesh):
    return jax.shard_map(
        body,
        mesh=mesh,
        in_specs=(
            P(None, "lev", "band", None, None),
            P(None, "lev", "band", None, None),
            P("band"),
            P(),
            P(),
            P(("band", "lev"), None, None),
            P(),
        ),
        out_specs=P(None, "lev", "band", None, None),
        check_vma=False,
    )
```

```python
import functools

import jax
import jax.numpy as jnp
import numpy as np
from jax import lax
from jax.experimental import pallas as pl
from jax.experimental.pallas import tpu as pltpu
from jax.sharding import PartitionSpec as P

LANES = 128
SPAN = 256
FINE = 16
SEATS = 4
UNROLL = 4
EACH = 4
SUB = 2
HALF_SPAN = SPAN // 2
SINE = [3.14159264, -5.16771008, 2.55007739, -0.59829041, 0.07765591]
COSINE = [0.99999995, -4.9347928, 4.05841079, -1.33187297, 0.21968242]


def halves(values):
    high = values.astype(jnp.bfloat16)
    return high, (values - high.astype(jnp.float32)).astype(jnp.bfloat16)


def iota(shape, dim):
    return lax.broadcasted_iota(jnp.int32, shape, dim)


def seat_of(field):
    return field % 2 * SEATS + field // 2 * 2


def turn(product, count, inverse):
    whole = jnp.floor(product * inverse + 0.5)
    part = (product - whole * count) * inverse
    square = part * part
    sine, cosine = SINE[-1], COSINE[-1]
    for term in SINE[-2::-1]:
        sine = sine * square + term
    for term in COSINE[-2::-1]:
        cosine = cosine * square + term
    sine = sine * part
    return 1.0 - 2.0 * sine * sine, 2.0 * sine * cosine


def dot(left, right):
    return lax.dot_general(
        left, right, (((1,), (0,)), ((), ())), preferred_element_type=jnp.float32
    )


def reverse(values):
    back = values.shape[1] - 1 - iota(values.shape, 1)
    return jnp.take_along_axis(values, back, axis=1, mode="promise_in_bounds")


def mirror(values):
    lane = iota(values.shape, 1)
    width = values.shape[1]
    return jnp.where(
        lane % 2 == 0,
        values + pltpu.roll(values, width - 1, 1),
        pltpu.roll(values, 1, 1) - values,
    )


def forward_kernel(
    counts, pairs, weights, field_ref, more_ref, out_ref, row_ref, high_ref, low_ref, wave_ref,
    *, stride,
):
    fields, local, _, _, length = field_ref.shape
    chunks, devices, tiles, lats, _ = out_ref.shape
    waves = length // 2
    rows = fields * local * 2
    each = 2 * local
    wide = 2 * each
    group = waves // 2 // devices // chunks
    blocks = length // SPAN
    each_step = field_ref.shape[2]

    def one(sub, carry):
        lat = pl.program_id(0) * each_step + sub
        count = counts[lat]
        real = 2.0 * count.astype(jnp.float32)
        inverse = 1.0 / jnp.full((1, 1), real, jnp.float32)
        for f in range(fields):
            for l in range(local):
                row_ref[pl.ds((f * local + l) * 2, 2), :] = field_ref[f, l, sub] + more_ref[f, l, sub]
        evens, odds = [], []
        for b in range(blocks):
            piece = row_ref[:, b * SPAN : (b + 1) * SPAN]
            place = b * SPAN + iota(piece.shape, 1)
            piece = jnp.where(place < count, piece, 0.0)
            right, left = piece[:, HALF_SPAN:], reverse(piece[:, :HALF_SPAN])
            evens.append(right + left)
            odds.append(right - left)
        even, even_low = halves(jnp.concatenate(evens, axis=0))
        odd, odd_low = halves(jnp.concatenate(odds, axis=0))
        evens = jnp.concatenate([even, even_low], axis=0)
        odds = jnp.concatenate([odd, odd_low], axis=0)
        total = blocks * rows
        weight = weights[lax.axis_index("band") * lats + lat]
        for q in range(waves // SPAN):
            order = q * SPAN + iota((1, SPAN), 1)
            order = order.astype(jnp.float32)
            steps = iota((FINE, SPAN), 0).astype(jnp.float32)
            fine_cos, fine_sin = turn((2.0 * steps + 1.0) * order, real, inverse)
            steps = steps[:8]
            coarse_cos, coarse_sin = turn(2 * FINE * steps * order, real, inverse)
            block_cos, block_sin = turn((2 * SPAN * steps + (SPAN - 1)) * order, real, inverse)
            for i in range(HALF_SPAN // FINE):
                cosine, sine = coarse_cos[i : i + 1], coarse_sin[i : i + 1]
                place = pl.ds(i * FINE, FINE)
                top, rest = halves(cosine * fine_cos - sine * fine_sin)
                high_ref[q, place, :SPAN] = top
                low_ref[q, place, :SPAN] = rest
                top, rest = halves(sine * fine_cos + cosine * fine_sin)
                high_ref[q, place, SPAN:] = top
                low_ref[q, place, SPAN:] = rest
            first = dot(evens, high_ref[q, :, :SPAN])
            with_cos = first[:total] + (first[total:] + dot(even, low_ref[q, :, :SPAN]))
            first = dot(odds, high_ref[q, :, SPAN:])
            with_sin = first[:total] + (first[total:] + dot(odd, low_ref[q, :, SPAN:]))
            real_part = jnp.zeros((rows, SPAN), jnp.float32)
            imaginary = jnp.zeros((rows, SPAN), jnp.float32)
            for b in range(blocks):
                in_cos = with_cos[b * rows : (b + 1) * rows]
                in_sin = with_sin[b * rows : (b + 1) * rows]
                cosine, sine = block_cos[b : b + 1], block_sin[b : b + 1]
                real_part += cosine * in_cos - sine * in_sin
                imaginary -= sine * in_cos + cosine * in_sin
            live = order.astype(jnp.int32) <= (count - 1) // 2
            scale = jnp.where(live, 2.0 * weight * inverse, 0.0)
            real_part, imaginary = real_part * scale, imaginary * scale
            parts = [jnp.zeros((wide, SPAN), jnp.float32)] * (LANES // wide)
            for f in range(fields):
                parts[seat_of(f)] = jnp.concatenate(
                    [real_part[f * each : (f + 1) * each], imaginary[f * each : (f + 1) * each]], axis=0
                )
            turned = jnp.concatenate(parts, axis=0).T
            wave_ref[pl.ds(q * SPAN * stride + lat, SPAN, stride=stride), :] = turned
        return carry

    lax.fori_loop(0, each_step, one, 0, unroll=SUB)

    @pl.when(pl.program_id(0) == pl.num_programs(0) - 1)
    def _():
        lane = iota((lats, LANES), 1) // wide

        def assemble(index, carry):
            chunk, device = index // devices, index % devices
            outs = [jnp.zeros((lats, LANES), jnp.float32)] * tiles
            for s in range(group):
                lower = pairs[device * chunks * group + chunk * group + s]
                for member in range(2):
                    wave = lower if member == 0 else waves - 1 - lower
                    value = wave_ref[pl.ds(wave * stride, lats), :]
                    moved = {}
                    for f in range(fields):
                        unit = member * fields + f
                        spot = unit % 2 * SEATS + s
                        step = (spot - seat_of(f)) * wide % LANES
                        if step not in moved:
                            moved[step] = pltpu.roll(value, step, 1)
                        outs[unit // 2] = jnp.where(lane == spot, moved[step], outs[unit // 2])
            for t in range(tiles):
                out_ref[chunk, device, t] = outs[t]
            return carry

        lax.fori_loop(0, devices * chunks, assemble, 0, unroll=UNROLL)


def inverse_kernel(
    counts, pairs, come_ref, out_ref, high_ref, low_ref, wave_ref, *, stride, light, short
):
    fields, local, _, _, length = out_ref.shape
    chunks, devices, tiles, lats, _ = come_ref.shape
    waves = length // 2
    rows = fields * local * 2
    each = 2 * local
    wide = 2 * each
    group = waves // 2 // devices // chunks
    blocks = length // SPAN
    each_step = out_ref.shape[2]

    @pl.when(pl.program_id(0) == 0)
    def _():
        lane = iota((lats, LANES), 1) // wide
        small = lax.axis_index("band") < light

        def spread(index, carry):
            chunk, device = index // devices, index % devices
            values = [come_ref[chunk, device, t] for t in range(tiles)]
            for t in range(short, tiles):
                values[t] = jnp.where(small, 0.0, values[t])
            for s in range(group):
                lower = pairs[device * chunks * group + chunk * group + s]
                for member in range(2):
                    wave = lower if member == 0 else waves - 1 - lower
                    out = jnp.zeros((lats, LANES), jnp.float32)
                    moved = {}
                    for f in range(fields):
                        unit = member * fields + f
                        spot = unit % 2 * SEATS + s
                        step = (seat_of(f) - spot) * wide % LANES
                        if (unit // 2, step) not in moved:
                            moved[unit // 2, step] = pltpu.roll(values[unit // 2], step, 1)
                        out = jnp.where(lane == seat_of(f), moved[unit // 2, step], out)
                    wave_ref[pl.ds(wave * stride, lats), :] = out
            return carry

        lax.fori_loop(0, devices * chunks, spread, 0, unroll=UNROLL)

    def one(sub, carry):
        lat = pl.program_id(0) * each_step + sub
        count = counts[lat]
        real = 2.0 * count.astype(jnp.float32)
        inverse = 1.0 / jnp.full((1, 1), real, jnp.float32)
        total = blocks * rows
        with_cos = jnp.zeros((total, HALF_SPAN), jnp.float32)
        with_sin = jnp.zeros((total, HALF_SPAN), jnp.float32)
        place = 2.0 * iota((1, HALF_SPAN), 1).astype(jnp.float32) + 1.0
        steps = iota((FINE, HALF_SPAN), 0).astype(jnp.float32)
        fine_cos, fine_sin = turn(steps * place, real, inverse)
        for q in range(waves // SPAN):
            start = q * SPAN
            coarse_cos, coarse_sin = turn((start + FINE * steps) * place, real, inverse)
            order = start + iota((1, SPAN), 1).astype(jnp.float32)
            rank = iota((8, SPAN), 0).astype(jnp.float32)
            block_cos, block_sin = turn((2 * SPAN * rank + (SPAN - 1)) * order, real, inverse)
            for i in range(SPAN // FINE):
                cosine, sine = coarse_cos[i : i + 1], coarse_sin[i : i + 1]
                part = pl.ds(i * FINE, FINE)
                top, rest = halves(cosine * fine_cos - sine * fine_sin)
                high_ref[q, 0, part] = top
                low_ref[q, 0, part] = rest
                top, rest = halves(sine * fine_cos + cosine * fine_sin)
                high_ref[q, 1, part] = top
                low_ref[q, 1, part] = rest
            turned = wave_ref[pl.ds(q * SPAN * stride + lat, SPAN, stride=stride), :].T
            real_part = jnp.concatenate(
                [turned[seat_of(f) * wide :][:each] for f in range(fields)], axis=0
            )
            imaginary = jnp.concatenate(
                [turned[seat_of(f) * wide + each :][:each] for f in range(fields)], axis=0
            )
            wave = order.astype(jnp.int32)
            double = jnp.where(wave == 0, 1.0, 2.0)
            double = jnp.where(wave <= (count - 1) // 2, double, 0.0)
            block_cos, block_sin = block_cos * double, block_sin * double
            evens, odds = [], []
            for b in range(blocks):
                cosine, sine = block_cos[b : b + 1], block_sin[b : b + 1]
                evens.append(real_part * cosine - imaginary * sine)
                odds.append(real_part * sine + imaginary * cosine)
            even, low = halves(jnp.concatenate(evens, axis=0))
            first = dot(jnp.concatenate([even, low], axis=0), high_ref[q, 0])
            with_cos += first[:total] + (first[total:] + dot(even, low_ref[q, 0]))
            odd, low = halves(jnp.concatenate(odds, axis=0))
            first = dot(jnp.concatenate([odd, low], axis=0), high_ref[q, 1])
            with_sin += first[:total] + (first[total:] + dot(odd, low_ref[q, 1]))
        right, left = with_cos - with_sin, reverse(with_cos + with_sin)
        for b in range(blocks):
            for part, side in ((0, left), (1, right)):
                start = b * SPAN + part * HALF_SPAN
                live = start + iota((rows, HALF_SPAN), 1) < count
                piece = jnp.where(live, side[b * rows : (b + 1) * rows], 0.0)
                for f in range(fields):
                    for l in range(local):
                        row = (f * local + l) * 2
                        out_ref[f, l, sub, :, start : start + HALF_SPAN] = piece[row : row + 2]
        return carry

    lax.fori_loop(0, each_step, one, 0, unroll=SUB)


def exchange_kernel(
    lowers, rates, sent_ref, table_ref, rank_ref, mine_ref, home_ref,
    come_ref, back_ref, pad_ref, data_ref, out_sem, in_sem, back_out_sem, back_in_sem, own_sem,
    *, lev, waves, light, short,
):
    slot = pl.program_id(0)
    chunks, devices, tiles, lats, _ = come_ref.shape
    bands = devices // lev
    slots = pl.num_programs(0)
    group = waves // 2 // devices // chunks
    chunk, spot = slot // group, slot % group
    band = lax.axis_index("band")
    me = band * lev + lax.axis_index("lev")

    def message(source, target, send_sem, recv_sem, g, there, where, device, small):
        part = pl.ds(0, short if small else tiles)
        return pltpu.make_async_remote_copy(
            src_ref=source.at[g, there, part],
            dst_ref=target.at[g, where, part],
            send_sem=send_sem.at[g, there],
            recv_sem=recv_sem.at[g, where],
            device_id=(device // lev, device % lev),
            device_id_type=pl.DeviceIdType.MESH,
        )

    def each_other(act, g, small_of):
        def one(step, carry):
            other = lax.rem(me + step, devices)
            small = small_of(other)

            @pl.when(small)
            def _():
                act(g, other, True)

            @pl.when(jnp.logical_not(small))
            def _():
                act(g, other, False)

            return carry

        lax.fori_loop(1, devices, one, 0)

    def mine_small(other):
        return band < light

    def their_small(other):
        return other // lev < light

    def go(g, other, small):
        message(sent_ref, come_ref, out_sem, in_sem, g, other, me, other, small).start()

    def gone(g, other, small):
        message(sent_ref, come_ref, out_sem, in_sem, g, other, me, other, small).wait_send()

    def come(g, other, small):
        message(sent_ref, come_ref, out_sem, in_sem, g, other, other, other, small).wait_recv()

    def back_go(g, other, small):
        message(back_ref, home_ref, back_out_sem, back_in_sem, g, other, me, other, small).start()

    def back_gone(g, other, small):
        message(back_ref, home_ref, back_out_sem, back_in_sem, g, other, me, other, small).wait_send()

    def back_come(g, other, small):
        message(
            back_ref, home_ref, back_out_sem, back_in_sem, g, other, other, other, small
        ).wait_recv()

    def own(g):
        return pltpu.make_async_copy(sent_ref.at[g, me], come_ref.at[g, me], own_sem.at[g])

    def own_back(g):
        return pltpu.make_async_copy(
            back_ref.at[g, me], home_ref.at[g, me], own_sem.at[chunks + g]
        )

    @pl.when(slot == 0)
    def _():
        def begin(g, carry):
            own(g).start()
            each_other(go, g, mine_small)
            return carry

        lax.fori_loop(0, chunks, begin, 0)
        pad_ref[...] = jnp.zeros_like(pad_ref)

    columns = table_ref.shape[1]
    pad_ref[:columns] = table_ref[0]
    table_high, table_low = halves(pad_ref[...])

    @pl.when(spot == 0)
    def _():
        own(chunk).wait()
        each_other(come, chunk, their_small)

    arrays = lev * tiles
    wides = -(-arrays // SEATS)
    width = wides * LANES
    member = LANES // (2 * SEATS)
    seat = iota((lats, LANES), 1) // member % SEATS
    for b in range(bands):
        for w in range(wides):
            value = jnp.zeros((lats, LANES), jnp.float32)
            for k in range(w * SEATS, min((w + 1) * SEATS, arrays)):
                if b < light and k % tiles >= short:
                    continue
                piece = come_ref[chunk, b * lev + k // tiles, k % tiles]
                shift = lax.rem((k % SEATS - spot) * member + LANES, LANES)
                value = jnp.where(seat == k % SEATS, pltpu.roll(piece, shift, 1), value)
            data_ref[pl.ds(b * lats, lats), w * LANES : (w + 1) * LANES] = value
    high, low = halves(mirror(data_ref[...]))
    first = dot(table_high, jnp.concatenate([high, low], axis=1))
    analysed = first[:, :width] + (first[:, width:] + dot(table_low, high))
    lower = lowers[slot]
    column = iota((pad_ref.shape[0], 1), 0)
    second = column >= waves - lower
    degree = jnp.where(second, column - 1, lower + column)
    order = jnp.where(second, waves - 1 - lower, lower)
    odd = (degree - order) & 1
    code = jnp.where(column <= waves, 2 * second.astype(jnp.int32) + odd, -1)
    degree = degree.astype(jnp.float32)
    ratio = degree * (degree + 1.0) * (1.0 / float((waves - 1) * waves))
    square = ratio * ratio
    rate = jnp.zeros(rank_ref.shape, jnp.float32)
    for r in range(rates.shape[0]):
        rate = jnp.where(rank_ref[...] == r, rates[r], rate)
    damped = jnp.where(code == mine_ref[...], analysed / (1.0 + rate * square), 0.0)
    high, low = halves(damped)
    first = dot(table_high.T, jnp.concatenate([high, low], axis=1))
    back = first[:, :width] + (first[:, width:] + dot(table_low.T, high))
    data_ref[...] = mirror(back)

    @pl.when(spot == 0)
    def _():
        back_ref[chunk] = jnp.zeros(back_ref.shape[1:], jnp.float32)

    for b in range(bands):
        for k in range(arrays):
            if b < light and k % tiles >= short:
                continue
            w = k // SEATS
            piece = data_ref[pl.ds(b * lats, lats), w * LANES : (w + 1) * LANES]
            shift = lax.rem((spot - k % SEATS) * member + LANES, LANES)
            target = (chunk, b * lev + k // tiles, k % tiles)
            back_ref[target] = jnp.where(seat == spot, pltpu.roll(piece, shift, 1), back_ref[target])

    @pl.when(spot == group - 1)
    def _():
        own_back(chunk).start()
        each_other(back_go, chunk, their_small)

    @pl.when(slot == slots - 1)
    def _():
        def end(g, carry):
            own_back(g).wait()
            each_other(back_come, g, mine_small)
            each_other(gone, g, mine_small)
            each_other(back_gone, g, their_small)
            return carry

        lax.fori_loop(0, chunks, end, 0)


def body(field_grid, increment, points, weights, pair_slot, legendre, strength):
    bands = lax.axis_size("band")
    lev = lax.axis_size("lev")
    devices = bands * lev
    fields, local, lats, _, length = field_grid.shape
    waves = length // 2
    slots, half, columns = legendre.shape
    member = 4 * local
    assert member * 2 * SEATS == LANES
    pair_count = waves // 2
    ranks = lax.iota(jnp.int32, pair_count)
    pairs = jnp.sum(jnp.where(pair_slot[None, :] == ranks[:, None], ranks[None, :], 0), axis=1)
    group = max(g for g in range(1, SEATS + 1) if slots % g == 0)
    chunks = slots // group
    tiles = fields
    short = (fields + 1) // 2
    most = [
        min(length, 48 + (length - 16) * (lats * (b + 1) - 1) // (half - 1)) for b in range(bands)
    ]
    light = sum((cells - 1) // 2 < pair_count for cells in most)
    stride = lats + 1 - lats % 2
    blocks = length // SPAN
    rows = fields * local * 2
    each_step = max(g for g in range(1, EACH + 1) if lats % g == 0)
    grid_block = pl.BlockSpec((fields, local, each_step, 2, length), lambda j, *_: (0, 0, j, 0, 0))
    buffer = (chunks, devices, tiles, lats, LANES)
    whole_block = pl.BlockSpec(buffer, lambda j, *_: (0, 0, 0, 0, 0))
    waved = pltpu.VMEM((waves * stride, LANES), jnp.float32)
    flops = lats * 6 * blocks * rows * SPAN * length
    sent = pl.pallas_call(
        functools.partial(forward_kernel, stride=stride),
        out_shape=jax.ShapeDtypeStruct(buffer, jnp.float32),
        grid_spec=pltpu.PrefetchScalarGridSpec(
            num_scalar_prefetch=3,
            grid=(lats // each_step,),
            in_specs=[grid_block, grid_block],
            out_specs=whole_block,
            scratch_shapes=[
                pltpu.VMEM((rows, length), jnp.float32),
                pltpu.VMEM((waves // SPAN, HALF_SPAN, 2 * SPAN), jnp.bfloat16),
                pltpu.VMEM((waves // SPAN, HALF_SPAN, 2 * SPAN), jnp.bfloat16),
                waved,
            ],
        ),
        cost_estimate=pl.CostEstimate(flops=flops, bytes_accessed=0, transcendentals=0),
    )(points, pairs, weights, field_grid, increment)

    arrays = lev * tiles
    width = -(-arrays // SEATS) * LANES
    padded = -(-columns // LANES) * LANES
    lane = np.arange(width)
    seat = lane % LANES // member
    array = lane // LANES * SEATS + seat % SEATS
    unit = array % tiles * 2 + seat // SEATS
    real = array < arrays
    mine = np.where(real, unit // fields * 2 + lane % 2, -2)
    level = array // tiles * local + lane // 2 % local
    rank = np.where(real, unit % fields * lev * local + level, 0)
    own = lax.dynamic_slice_in_dim(pairs, lax.axis_index(("band", "lev")) * slots, slots)
    home = pl.pallas_call(
        functools.partial(exchange_kernel, lev=lev, waves=waves, light=light, short=short),
        out_shape=jax.ShapeDtypeStruct(buffer, jnp.float32),
        grid_spec=pltpu.PrefetchScalarGridSpec(
            num_scalar_prefetch=2,
            grid=(slots,),
            in_specs=[
                pl.BlockSpec(memory_space=pl.ANY),
                pl.BlockSpec((1, columns, half), lambda s, *_: (s, 0, 0)),
                pl.BlockSpec((1, width), lambda s, *_: (0, 0)),
                pl.BlockSpec((1, width), lambda s, *_: (0, 0)),
            ],
            out_specs=pl.BlockSpec(memory_space=pl.ANY),
            scratch_shapes=[
                pltpu.VMEM(buffer, jnp.float32),
                pltpu.VMEM(buffer, jnp.float32),
                pltpu.VMEM((padded, half), jnp.float32),
                pltpu.VMEM((half, width), jnp.float32),
                pltpu.SemaphoreType.DMA((chunks, devices)),
                pltpu.SemaphoreType.DMA((chunks, devices)),
                pltpu.SemaphoreType.DMA((chunks, devices)),
                pltpu.SemaphoreType.DMA((chunks, devices)),
                pltpu.SemaphoreType.DMA((2 * chunks,)),
            ],
        ),
        compiler_params=pltpu.CompilerParams(has_side_effects=True),
        cost_estimate=pl.CostEstimate(
            flops=slots * 12 * half * padded * width, bytes_accessed=0, transcendentals=0
        ),
    )(
        own,
        strength.reshape(-1),
        sent,
        jnp.swapaxes(legendre, 1, 2),
        jnp.asarray(rank[None, :], jnp.int32),
        jnp.asarray(mine[None, :], jnp.int32),
    )

    return pl.pallas_call(
        functools.partial(inverse_kernel, stride=stride, light=light, short=short),
        out_shape=jax.ShapeDtypeStruct(field_grid.shape, jnp.float32),
        grid_spec=pltpu.PrefetchScalarGridSpec(
            num_scalar_prefetch=2,
            grid=(lats // each_step,),
            in_specs=[whole_block],
            out_specs=grid_block,
            scratch_shapes=[
                pltpu.VMEM((waves // SPAN, 2, SPAN, HALF_SPAN), jnp.bfloat16),
                pltpu.VMEM((waves // SPAN, 2, SPAN, HALF_SPAN), jnp.bfloat16),
                waved,
            ],
        ),
        cost_estimate=pl.CostEstimate(flops=flops, bytes_accessed=0, transcendentals=0),
    )(points, pairs, home)


def solution(mesh):
    return jax.shard_map(
        body,
        mesh=mesh,
        in_specs=(
            P(None, "lev", "band", None, None),
            P(None, "lev", "band", None, None),
            P("band"),
            P(),
            P(),
            P(("band", "lev"), None, None),
            P(),
        ),
        out_specs=P(None, "lev", "band", None, None),
        check_vma=False,
    )
```

```python
import functools

import jax
import jax.numpy as jnp
import numpy as np
from jax import lax
from jax.experimental import pallas as pl
from jax.experimental.pallas import tpu as pltpu
from jax.sharding import PartitionSpec as P

LANES = 128
SPAN = 256
FINE = 16
SEATS = 4
UNROLL = 4
EACH = 4
SUB = 2
HALF_SPAN = SPAN // 2
SINE = [3.14159264, -5.16771008, 2.55007739, -0.59829041, 0.07765591]
COSINE = [0.99999995, -4.9347928, 4.05841079, -1.33187297, 0.21968242]


def halves(values):
    high = values.astype(jnp.bfloat16)
    return high, (values - high.astype(jnp.float32)).astype(jnp.bfloat16)


def iota(shape, dim):
    return lax.broadcasted_iota(jnp.int32, shape, dim)


def seat_of(field):
    return field % 2 * SEATS + field // 2 * 2


def turn(product, count, inverse):
    whole = jnp.floor(product * inverse + 0.5)
    part = (product - whole * count) * inverse
    square = part * part
    sine, cosine = SINE[-1], COSINE[-1]
    for term in SINE[-2::-1]:
        sine = sine * square + term
    for term in COSINE[-2::-1]:
        cosine = cosine * square + term
    sine = sine * part
    return 1.0 - 2.0 * sine * sine, 2.0 * sine * cosine


def dot(left, right):
    return lax.dot_general(
        left, right, (((1,), (0,)), ((), ())), preferred_element_type=jnp.float32
    )


def reverse(values):
    back = values.shape[1] - 1 - iota(values.shape, 1)
    return jnp.take_along_axis(values, back, axis=1, mode="promise_in_bounds")


def mirror(values):
    lane = iota(values.shape, 1)
    width = values.shape[1]
    return jnp.where(
        lane % 2 == 0,
        values + pltpu.roll(values, width - 1, 1),
        pltpu.roll(values, 1, 1) - values,
    )


def forward_step(
    step, group_steps, finish,
    counts, pairs, weights, field_ref, more_ref, out_ref, row_ref, high_ref, low_ref, wave_ref,
    *, stride, lats, sets,
):
    fields, local, _, _, length = field_ref.shape
    chunks, devices, tiles, _, _ = out_ref.shape
    each_set = lats // sets
    waves = length // 2
    rows = fields * local * 2
    each = 2 * local
    wide = 2 * each
    group = waves // 2 // devices // chunks
    blocks = length // SPAN
    each_step = field_ref.shape[2]

    def one(sub, carry):
        lat = step * each_step + sub
        count = counts[lat]
        real = 2.0 * count.astype(jnp.float32)
        inverse = 1.0 / jnp.full((1, 1), real, jnp.float32)
        for f in range(fields):
            for l in range(local):
                row_ref[pl.ds((f * local + l) * 2, 2), :] = field_ref[f, l, sub] + more_ref[f, l, sub]
        evens, odds = [], []
        for b in range(blocks):
            piece = row_ref[:, b * SPAN : (b + 1) * SPAN]
            place = b * SPAN + iota(piece.shape, 1)
            piece = jnp.where(place < count, piece, 0.0)
            right, left = piece[:, HALF_SPAN:], reverse(piece[:, :HALF_SPAN])
            evens.append(right + left)
            odds.append(right - left)
        even, even_low = halves(jnp.concatenate(evens, axis=0))
        odd, odd_low = halves(jnp.concatenate(odds, axis=0))
        evens = jnp.concatenate([even, even_low], axis=0)
        odds = jnp.concatenate([odd, odd_low], axis=0)
        total = blocks * rows
        weight = weights[lax.axis_index("band") * lats + lat]
        for q in range(waves // SPAN):
            order = q * SPAN + iota((1, SPAN), 1)
            order = order.astype(jnp.float32)
            steps = iota((FINE, SPAN), 0).astype(jnp.float32)
            fine_cos, fine_sin = turn((2.0 * steps + 1.0) * order, real, inverse)
            steps = steps[:8]
            coarse_cos, coarse_sin = turn(2 * FINE * steps * order, real, inverse)
            block_cos, block_sin = turn((2 * SPAN * steps + (SPAN - 1)) * order, real, inverse)
            for i in range(HALF_SPAN // FINE):
                cosine, sine = coarse_cos[i : i + 1], coarse_sin[i : i + 1]
                place = pl.ds(i * FINE, FINE)
                top, rest = halves(cosine * fine_cos - sine * fine_sin)
                high_ref[q, place, :SPAN] = top
                low_ref[q, place, :SPAN] = rest
                top, rest = halves(sine * fine_cos + cosine * fine_sin)
                high_ref[q, place, SPAN:] = top
                low_ref[q, place, SPAN:] = rest
            first = dot(evens, high_ref[q, :, :SPAN])
            with_cos = first[:total] + (first[total:] + dot(even, low_ref[q, :, :SPAN]))
            first = dot(odds, high_ref[q, :, SPAN:])
            with_sin = first[:total] + (first[total:] + dot(odd, low_ref[q, :, SPAN:]))
            real_part = jnp.zeros((rows, SPAN), jnp.float32)
            imaginary = jnp.zeros((rows, SPAN), jnp.float32)
            for b in range(blocks):
                in_cos = with_cos[b * rows : (b + 1) * rows]
                in_sin = with_sin[b * rows : (b + 1) * rows]
                cosine, sine = block_cos[b : b + 1], block_sin[b : b + 1]
                real_part += cosine * in_cos - sine * in_sin
                imaginary -= sine * in_cos + cosine * in_sin
            live = order.astype(jnp.int32) <= (count - 1) // 2
            scale = jnp.where(live, 2.0 * weight * inverse, 0.0)
            real_part, imaginary = real_part * scale, imaginary * scale
            parts = [jnp.zeros((wide, SPAN), jnp.float32)] * (LANES // wide)
            for f in range(fields):
                parts[seat_of(f)] = jnp.concatenate(
                    [real_part[f * each : (f + 1) * each], imaginary[f * each : (f + 1) * each]], axis=0
                )
            turned = jnp.concatenate(parts, axis=0).T
            wave_ref[pl.ds(q * SPAN * stride + lat % each_set, SPAN, stride=stride), :] = turned
        return carry

    lax.fori_loop(0, each_step, one, 0, unroll=SUB)

    @pl.when(step % group_steps == group_steps - 1)
    def _():
        part = step // group_steps
        lane = iota((each_set, LANES), 1) // wide

        def assemble(index, carry):
            chunk, device = index // devices, index % devices
            outs = [jnp.zeros((each_set, LANES), jnp.float32)] * tiles
            for s in range(group):
                lower = pairs[device * chunks * group + chunk * group + s]
                for member in range(2):
                    wave = lower if member == 0 else waves - 1 - lower
                    value = wave_ref[pl.ds(wave * stride, each_set), :]
                    moved = {}
                    for f in range(fields):
                        unit = member * fields + f
                        spot = unit % 2 * SEATS + s
                        step = (spot - seat_of(f)) * wide % LANES
                        if step not in moved:
                            moved[step] = pltpu.roll(value, step, 1)
                        outs[unit // 2] = jnp.where(lane == spot, moved[step], outs[unit // 2])
            for t in range(tiles):
                out_ref[chunk, device, t, pl.ds(part * each_set, each_set)] = outs[t]
            return carry

        lax.fori_loop(0, devices * chunks, assemble, 0, unroll=UNROLL)
        finish(part)


def inverse_tables(count, high_ref, low_ref):
    real = 2.0 * count.astype(jnp.float32)
    inverse = 1.0 / jnp.full((1, 1), real, jnp.float32)
    place = 2.0 * iota((1, HALF_SPAN), 1).astype(jnp.float32) + 1.0
    steps = iota((FINE, HALF_SPAN), 0).astype(jnp.float32)
    fine_cos, fine_sin = turn(steps * place, real, inverse)
    for q in range(high_ref.shape[1]):
        coarse_cos, coarse_sin = turn((q * SPAN + FINE * steps) * place, real, inverse)
        for i in range(SPAN // FINE):
            cosine, sine = coarse_cos[i : i + 1], coarse_sin[i : i + 1]
            part = pl.ds(i * FINE, FINE)
            top, rest = halves(cosine * fine_cos - sine * fine_sin)
            high_ref[0, q, 0, part] = top
            low_ref[0, q, 0, part] = rest
            top, rest = halves(sine * fine_cos + cosine * fine_sin)
            high_ref[0, q, 1, part] = top
            low_ref[0, q, 1, part] = rest


def inverse_kernel(
    counts, pairs, come_ref, high_ref, low_ref, out_ref, wave_ref, *, stride, light, short
):
    fields, local, _, _, length = out_ref.shape
    chunks, devices, tiles, lats, _ = come_ref.shape
    waves = length // 2
    rows = fields * local * 2
    each = 2 * local
    wide = 2 * each
    group = waves // 2 // devices // chunks
    blocks = length // SPAN
    each_step = out_ref.shape[2]

    @pl.when(pl.program_id(0) == 0)
    def _():
        lane = iota((lats, LANES), 1) // wide
        small = lax.axis_index("band") < light

        def spread(index, carry):
            chunk, device = index // devices, index % devices
            values = [come_ref[chunk, device, t] for t in range(tiles)]
            for t in range(short, tiles):
                values[t] = jnp.where(small, 0.0, values[t])
            for s in range(group):
                lower = pairs[device * chunks * group + chunk * group + s]
                for member in range(2):
                    wave = lower if member == 0 else waves - 1 - lower
                    out = jnp.zeros((lats, LANES), jnp.float32)
                    moved = {}
                    for f in range(fields):
                        unit = member * fields + f
                        spot = unit % 2 * SEATS + s
                        step = (seat_of(f) - spot) * wide % LANES
                        if (unit // 2, step) not in moved:
                            moved[unit // 2, step] = pltpu.roll(values[unit // 2], step, 1)
                        out = jnp.where(lane == seat_of(f), moved[unit // 2, step], out)
                    wave_ref[pl.ds(wave * stride, lats), :] = out
            return carry

        lax.fori_loop(0, devices * chunks, spread, 0, unroll=UNROLL)

    def one(sub, carry):
        lat = pl.program_id(0) * each_step + sub
        count = counts[lat]
        real = 2.0 * count.astype(jnp.float32)
        inverse = 1.0 / jnp.full((1, 1), real, jnp.float32)
        total = blocks * rows
        with_cos = jnp.zeros((total, HALF_SPAN), jnp.float32)
        with_sin = jnp.zeros((total, HALF_SPAN), jnp.float32)
        for q in range(waves // SPAN):
            start = q * SPAN
            order = start + iota((1, SPAN), 1).astype(jnp.float32)
            rank = iota((8, SPAN), 0).astype(jnp.float32)
            block_cos, block_sin = turn((2 * SPAN * rank + (SPAN - 1)) * order, real, inverse)
            turned = wave_ref[pl.ds(q * SPAN * stride + lat, SPAN, stride=stride), :].T
            real_part = jnp.concatenate(
                [turned[seat_of(f) * wide :][:each] for f in range(fields)], axis=0
            )
            imaginary = jnp.concatenate(
                [turned[seat_of(f) * wide + each :][:each] for f in range(fields)], axis=0
            )
            wave = order.astype(jnp.int32)
            double = jnp.where(wave == 0, 1.0, 2.0)
            double = jnp.where(wave <= (count - 1) // 2, double, 0.0)
            block_cos, block_sin = block_cos * double, block_sin * double
            evens, odds = [], []
            for b in range(blocks):
                cosine, sine = block_cos[b : b + 1], block_sin[b : b + 1]
                evens.append(real_part * cosine - imaginary * sine)
                odds.append(real_part * sine + imaginary * cosine)
            even, low = halves(jnp.concatenate(evens, axis=0))
            first = dot(jnp.concatenate([even, low], axis=0), high_ref[sub, q, 0])
            with_cos += first[:total] + (first[total:] + dot(even, low_ref[sub, q, 0]))
            odd, low = halves(jnp.concatenate(odds, axis=0))
            first = dot(jnp.concatenate([odd, low], axis=0), high_ref[sub, q, 1])
            with_sin += first[:total] + (first[total:] + dot(odd, low_ref[sub, q, 1]))
        right, left = with_cos - with_sin, reverse(with_cos + with_sin)
        for b in range(blocks):
            for part, side in ((0, left), (1, right)):
                start = b * SPAN + part * HALF_SPAN
                live = start + iota((rows, HALF_SPAN), 1) < count
                piece = jnp.where(live, side[b * rows : (b + 1) * rows], 0.0)
                for f in range(fields):
                    for l in range(local):
                        row = (f * local + l) * 2
                        out_ref[f, l, sub, :, start : start + HALF_SPAN] = piece[row : row + 2]
        return carry

    lax.fori_loop(0, each_step, one, 0, unroll=SUB)


def exchange_kernel(
    counts, pairs, weights, lowers, rates, field_ref, more_ref, table_ref, rank_ref, mine_ref,
    home_ref, top_ref, rest_ref, row_ref, high_ref, low_ref, wave_ref, sent_ref, come_ref, back_ref, pad_ref,
    data_ref, out_sem, in_sem, back_out_sem, back_in_sem, own_sem,
    *, lev, waves, light, short, stride, lat_steps, sets,
):
    step = pl.program_id(0)
    slot = step - lat_steps
    chunks, devices, tiles, lats, _ = come_ref.shape
    each_set = lats // sets
    bands = devices // lev
    slots = pl.num_programs(0) - lat_steps - lats
    group = waves // 2 // devices // chunks
    chunk, spot = slot // group, slot % group
    band = lax.axis_index("band")
    me = band * lev + lax.axis_index("lev")

    def copy(source, target, send_sem, recv_sem, device):
        return pltpu.make_async_remote_copy(
            src_ref=source,
            dst_ref=target,
            send_sem=send_sem,
            recv_sem=recv_sem,
            device_id=(device // lev, device % lev),
            device_id_type=pl.DeviceIdType.MESH,
        )

    def message(n, there, where, device, small, split):
        part = pl.ds(0, short if small else tiles)
        g, rows = (0, pl.ds(n * each_set, each_set)) if split else (n - sets + 1, pl.ds(0, lats))
        return copy(
            sent_ref.at[g, there, part, rows], come_ref.at[g, where, part, rows],
            out_sem.at[n, there], in_sem.at[n, where], device,
        )

    def answer(g, there, where, device, small):
        part = pl.ds(0, short if small else tiles)
        return copy(
            back_ref.at[g, there, part], home_ref.at[g, where, part],
            back_out_sem.at[g, there], back_in_sem.at[g, where], device,
        )

    def each_other(act, g, small_of):
        def one(hop, carry):
            other = lax.rem(me + hop, devices)
            small = small_of(other)

            @pl.when(small)
            def _():
                act(g, other, True)

            @pl.when(jnp.logical_not(small))
            def _():
                act(g, other, False)

            return carry

        lax.fori_loop(1, devices, one, 0)

    def mine_small(other):
        return band < light

    def their_small(other):
        return other // lev < light

    def back_go(g, other, small):
        answer(g, other, me, other, small).start()

    def back_gone(g, other, small):
        answer(g, other, me, other, small).wait_send()

    def back_come(g, other, small):
        answer(g, other, other, other, small).wait_recv()

    def own_back(g):
        return pltpu.make_async_copy(back_ref.at[g, me], home_ref.at[g, me], own_sem.at[g])

    def send(n, split):
        def act(n, other, small):
            message(n, other, me, other, small, split).start()

        each_other(act, n, mine_small)

    def arrive(n, split):
        def act(n, other, small):
            message(n, other, other, other, small, split).wait_recv()

        each_other(act, n, their_small)

    def leave(n, split):
        def act(n, other, small):
            message(n, other, me, other, small, split).wait_send()

        each_other(act, n, mine_small)

    def all_of(act, first, last, split):
        lax.fori_loop(first, last, lambda n, carry: (act(n, split), carry)[1], 0)

    def finish(part):
        send(part, True)

        @pl.when(part == sets - 1)
        def _():
            all_of(send, sets, sets + chunks - 1, False)

    def legendre():
        columns = table_ref.shape[1]
        pad_ref[:columns] = table_ref[0]
        table_high, table_low = halves(pad_ref[...])

        @pl.when(slot == 0)
        def _():
            all_of(arrive, 0, sets, True)

        @pl.when((slot > 0) & (spot == 0))
        def _():
            arrive(chunk + sets - 1, False)

        arrays = lev * tiles
        wides = -(-arrays // SEATS)
        width = wides * LANES
        member = LANES // (2 * SEATS)
        seat = iota((lats, LANES), 1) // member % SEATS
        for b in range(bands):
            for w in range(wides):
                value = jnp.zeros((lats, LANES), jnp.float32)
                for k in range(w * SEATS, min((w + 1) * SEATS, arrays)):
                    if b < light and k % tiles >= short:
                        continue
                    piece = come_ref[chunk, b * lev + k // tiles, k % tiles]
                    shift = lax.rem((k % SEATS - spot) * member + LANES, LANES)
                    value = jnp.where(seat == k % SEATS, pltpu.roll(piece, shift, 1), value)
                rows = pl.ds(b * lats, lats)
                data_ref[rows, w * LANES : (w + 1) * LANES] = value
        high, low = halves(mirror(data_ref[...]))
        first = dot(table_high, jnp.concatenate([high, low], axis=1))
        analysed = first[:, :width] + (first[:, width:] + dot(table_low, high))
        lower = lowers[slot]
        column = iota((pad_ref.shape[0], 1), 0)
        second = column >= waves - lower
        degree = jnp.where(second, column - 1, lower + column)
        order = jnp.where(second, waves - 1 - lower, lower)
        odd = (degree - order) & 1
        code = jnp.where(column <= waves, 2 * second.astype(jnp.int32) + odd, -1)
        degree = degree.astype(jnp.float32)
        ratio = degree * (degree + 1.0) * (1.0 / float((waves - 1) * waves))
        square = ratio * ratio
        rate = jnp.zeros(rank_ref.shape, jnp.float32)
        for r in range(rates.shape[0]):
            rate = jnp.where(rank_ref[...] == r, rates[r], rate)
        damped = jnp.where(code == mine_ref[...], analysed / (1.0 + rate * square), 0.0)
        high, low = halves(damped)
        first = dot(table_high.T, jnp.concatenate([high, low], axis=1))
        back = first[:, :width] + (first[:, width:] + dot(table_low.T, high))
        data_ref[...] = mirror(back)

        @pl.when(spot == 0)
        def _():
            back_ref[chunk] = jnp.zeros(back_ref.shape[1:], jnp.float32)

        for b in range(bands):
            for k in range(arrays):
                if b < light and k % tiles >= short:
                    continue
                w = k // SEATS
                piece = data_ref[pl.ds(b * lats, lats), w * LANES : (w + 1) * LANES]
                shift = lax.rem((spot - k % SEATS) * member + LANES, LANES)
                target = (chunk, b * lev + k // tiles, k % tiles)
                back_ref[target] = jnp.where(seat == spot, pltpu.roll(piece, shift, 1), back_ref[target])

        @pl.when(spot == group - 1)
        def _():
            own_back(chunk).start()
            each_other(back_go, chunk, their_small)

    @pl.when(step < lat_steps)
    def _():
        forward_step(
            step, lat_steps // sets, finish,
            counts, pairs, weights, field_ref, more_ref, sent_ref,
            row_ref, high_ref, low_ref, wave_ref, stride=stride, lats=lats, sets=sets,
        )

    @pl.when(slot == 0)
    def _():
        pad_ref[...] = jnp.zeros_like(pad_ref)
        for g in range(chunks):
            come_ref[g, me] = sent_ref[g, me]

    @pl.when((slot >= 0) & (slot < slots))
    def _():
        legendre()

    @pl.when(slot >= slots)
    def _():
        inverse_tables(counts[slot - slots], top_ref, rest_ref)

    @pl.when(slot == slots + lats - 1)
    def _():
        def end(g, carry):
            own_back(g).wait()
            each_other(back_come, g, mine_small)
            each_other(back_gone, g, their_small)
            return carry

        lax.fori_loop(0, chunks, end, 0)
        all_of(leave, 0, sets, True)
        all_of(leave, sets, sets + chunks - 1, False)


def body(field_grid, increment, points, weights, pair_slot, legendre, strength):
    bands = lax.axis_size("band")
    lev = lax.axis_size("lev")
    devices = bands * lev
    fields, local, lats, _, length = field_grid.shape
    waves = length // 2
    slots, half, columns = legendre.shape
    member = 4 * local
    assert member * 2 * SEATS == LANES
    pair_count = waves // 2
    ranks = lax.iota(jnp.int32, pair_count)
    pairs = jnp.sum(jnp.where(pair_slot[None, :] == ranks[:, None], ranks[None, :], 0), axis=1)
    group = max(g for g in range(1, SEATS + 1) if slots % g == 0)
    chunks = slots // group
    tiles = fields
    short = (fields + 1) // 2
    most = [
        min(length, 48 + (length - 16) * (lats * (b + 1) - 1) // (half - 1)) for b in range(bands)
    ]
    light = sum((cells - 1) // 2 < pair_count for cells in most)
    stride = lats + 1 - lats % 2
    each_set = 8 if lats % 8 == 0 else lats
    sets = lats // each_set
    set_stride = each_set + 1 - each_set % 2
    blocks = length // SPAN
    rows = fields * local * 2
    each_step = max(g for g in range(1, EACH + 1) if each_set % g == 0)
    lat_steps = lats // each_step
    grid_block = pl.BlockSpec((fields, local, each_step, 2, length), lambda j, *_: (0, 0, j, 0, 0))
    buffer = (chunks, devices, tiles, lats, LANES)
    early_block = pl.BlockSpec(
        (fields, local, each_step, 2, length),
        lambda s, *_: (0, 0, jnp.minimum(s, lat_steps - 1), 0, 0),
    )
    whole_block = pl.BlockSpec(buffer, lambda j, *_: (0, 0, 0, 0, 0))
    waved = pltpu.VMEM((waves * stride, LANES), jnp.float32)
    flops = lats * 6 * blocks * rows * SPAN * length
    arrays = lev * tiles
    width = -(-arrays // SEATS) * LANES
    padded = -(-columns // LANES) * LANES
    lane = np.arange(width)
    seat = lane % LANES // member
    array = lane // LANES * SEATS + seat % SEATS
    unit = array % tiles * 2 + seat // SEATS
    real = array < arrays
    mine = np.where(real, unit // fields * 2 + lane % 2, -2)
    level = array // tiles * local + lane // 2 % local
    rank = np.where(real, unit % fields * lev * local + level, 0)
    own = lax.dynamic_slice_in_dim(pairs, lax.axis_index(("band", "lev")) * slots, slots)
    turns = (waves // SPAN, 2, SPAN, HALF_SPAN)
    home, top, rest = pl.pallas_call(
        functools.partial(
            exchange_kernel, lev=lev, waves=waves, light=light, short=short,
            stride=set_stride, lat_steps=lat_steps, sets=sets,
        ),
        out_shape=[jax.ShapeDtypeStruct(buffer, jnp.float32)]
        + [jax.ShapeDtypeStruct((lats, *turns), jnp.bfloat16)] * 2,
        grid_spec=pltpu.PrefetchScalarGridSpec(
            num_scalar_prefetch=5,
            grid=(lat_steps + slots + lats,),
            in_specs=[
                early_block,
                early_block,
                pl.BlockSpec(
                    (1, columns, half), lambda s, *_: (jnp.clip(s - lat_steps, 0, slots - 1), 0, 0)
                ),
                pl.BlockSpec((1, width), lambda s, *_: (0, 0)),
                pl.BlockSpec((1, width), lambda s, *_: (0, 0)),
            ],
            out_specs=[pl.BlockSpec(memory_space=pl.ANY)]
            + [
                pl.BlockSpec(
                    (1, *turns),
                    lambda s, *_: (jnp.maximum(s - lat_steps - slots, 0), 0, 0, 0, 0),
                )
            ]
            * 2,
            scratch_shapes=[
                pltpu.VMEM((rows, length), jnp.float32),
                pltpu.VMEM((waves // SPAN, HALF_SPAN, 2 * SPAN), jnp.bfloat16),
                pltpu.VMEM((waves // SPAN, HALF_SPAN, 2 * SPAN), jnp.bfloat16),
                pltpu.VMEM((waves * set_stride, LANES), jnp.float32),
                pltpu.VMEM(buffer, jnp.float32),
                pltpu.VMEM(buffer, jnp.float32),
                pltpu.VMEM(buffer, jnp.float32),
                pltpu.VMEM((padded, half), jnp.float32),
                pltpu.VMEM((half, width), jnp.float32),
                pltpu.SemaphoreType.DMA((sets + chunks - 1, devices)),
                pltpu.SemaphoreType.DMA((sets + chunks - 1, devices)),
                pltpu.SemaphoreType.DMA((chunks, devices)),
                pltpu.SemaphoreType.DMA((chunks, devices)),
                pltpu.SemaphoreType.DMA((chunks,)),
            ],
        ),
        compiler_params=pltpu.CompilerParams(has_side_effects=True),
        cost_estimate=pl.CostEstimate(
            flops=slots * 12 * half * padded * width, bytes_accessed=0, transcendentals=0
        ),
    )(
        points,
        pairs,
        weights,
        own,
        strength.reshape(-1),
        field_grid,
        increment,
        jnp.swapaxes(legendre, 1, 2),
        jnp.asarray(rank[None, :], jnp.int32),
        jnp.asarray(mine[None, :], jnp.int32),
    )

    return pl.pallas_call(
        functools.partial(inverse_kernel, stride=stride, light=light, short=short),
        out_shape=jax.ShapeDtypeStruct(field_grid.shape, jnp.float32),
        grid_spec=pltpu.PrefetchScalarGridSpec(
            num_scalar_prefetch=2,
            grid=(lats // each_step,),
            in_specs=[whole_block]
            + [pl.BlockSpec((each_step, *turns), lambda j, *_: (j, 0, 0, 0, 0))] * 2,
            out_specs=grid_block,
            scratch_shapes=[
                waved,
            ],
        ),
        cost_estimate=pl.CostEstimate(flops=flops, bytes_accessed=0, transcendentals=0),
    )(points, pairs, home, top, rest)


def solution(mesh):
    return jax.shard_map(
        body,
        mesh=mesh,
        in_specs=(
            P(None, "lev", "band", None, None),
            P(None, "lev", "band", None, None),
            P("band"),
            P(),
            P(),
            P(("band", "lev"), None, None),
            P(),
        ),
        out_specs=P(None, "lev", "band", None, None),
        check_vma=False,
    )
```
